32 devices in a mesh: gx: 2 (over core), gy: 4 (over y, x), gz: 4 (over z).
Axes of the slice: x: 2, y: 2, z: 4, core: 2. Of those that a mesh axis runs over, the one named last changes fastest.
Arguments:
- field: float32 [256, 1024, 512], P('gz', 'gx', 'gy'), may hold values from -48 to 48
- factor_a: float32 [1024, 1024], replicated, may hold values from -0.5 to 3.5
- factor_b: float32 [512, 512], replicated, may hold values from -0.5 to 3.5
- factor_c: float32 [256, 256], replicated, may hold values from -0.5 to 3.5
Outputs:
- propagated: float32 [256, 1024, 512], P('gz', 'gx', 'gy')
The draws below stay inside these ranges and needn't reach their ends.
All inputs are finite; a program needn't handle non-finite values.
Results may differ from the reference program's by a relative error of at most 0.00007.
Values sent between devices are 32-bit elements; how exact they have to be, the bound alone decides.
A program may use at most 192 MiB of HBM per device.

```python
import math
import jax
import jax.numpy as jnp
from jax import lax

N1 = 1024
N2 = 512
N3 = 256


def draw_field(key, part):
    keys = jax.random.split(jax.random.fold_in(key, 10), 4)
    spread = math.log(2.2)
    rising = 0.5 * math.log(3.0)
    scale_three = jnp.exp(jax.random.uniform(keys[0], (N3,), jnp.float32, 0.0, spread) + rising * jnp.arange(N3, dtype=jnp.float32) / N3)
    scale_one = jnp.exp(jax.random.uniform(keys[1], (N1,), jnp.float32, 0.0, spread) + rising * jnp.arange(N1, dtype=jnp.float32) / N1)
    scale_two = jnp.exp(jax.random.uniform(keys[2], (N2,), jnp.float32, 0.0, spread) + rising * jnp.arange(N2, dtype=jnp.float32) / N2)
    noise = jax.random.truncated_normal(keys[3], -6.0, 6.0, (N3, N1, N2), jnp.float32)
    values = 0.25 * noise * scale_three[:, None, None] * scale_one[None, :, None] * scale_two[None, None, :]
    return jnp.clip(values, -48.0, 48.0)


def make_factor(key, order):
    keys = jax.random.split(key, 2)
    diagonal = jnp.exp(jax.random.uniform(keys[0], (order,), jnp.float32, 0.0, math.log(3.0)))
    off_part = jax.random.truncated_normal(keys[1], -4.0, 4.0, (order, order), jnp.float32) * 0.6 * order ** (-0.5)
    return off_part + jnp.diag(diagonal)


def draw_factor_a(key, part):
    return make_factor(jax.random.fold_in(key, 11), N1)


def draw_factor_b(key, part):
    return make_factor(jax.random.fold_in(key, 12), N2)


def draw_factor_c(key, part):
    return make_factor(jax.random.fold_in(key, 13), N3)


def setup_inputs(seed: int = 0) -> dict:
    splits = jax.random.split(jax.random.key(seed), 5)
    field = draw_field(jax.random.fold_in(splits[4], 71), 0)
    factor_a = draw_factor_a(jax.random.fold_in(splits[4], 71), 0)
    factor_b = draw_factor_b(jax.random.fold_in(splits[4], 71), 0)
    factor_c = draw_factor_c(jax.random.fold_in(splits[4], 71), 0)
    return {"field": field, "factor_a": factor_a, "factor_b": factor_b, "factor_c": factor_c}


epsilon = 1e-06
target_ratio = 0.5

def apply_operator(tensor, factor_a, factor_b, factor_c):
    highest = lax.Precision.HIGHEST
    along_one = jnp.einsum('ip,kpj->kij', factor_a, tensor, precision=highest)
    along_two = jnp.einsum('kip,jp->kij', tensor, factor_b, precision=highest)
    along_three = jnp.einsum('kp,pij->kij', factor_c, tensor, precision=highest)
    return along_one + along_two + along_three

def reference(field, factor_a, factor_b, factor_c):
    first_term = apply_operator(field, factor_a, factor_b, factor_c)
    size_field = jnp.sum(field * field)
    size_first = jnp.sum(first_term * first_term)
    step = target_ratio * jnp.sqrt(size_field / (size_first + epsilon))
    second_term = apply_operator(first_term, factor_a, factor_b, factor_c)
    return field - step * first_term + step * step / 2.0 * second_term
```

```python
import functools

import jax
import jax.numpy as jnp
from jax import lax
from jax.experimental import pallas as pl
from jax.experimental.pallas import tpu as pltpu
from jax.sharding import PartitionSpec as P

epsilon = 1e-06
target_ratio = 0.5
slots = 4
ring = 8
hold = 3
late = 2
F32 = jnp.float32
MESH = pl.DeviceIdType.MESH


def halves(x):
    top = lax.reduce_precision(x, 8, 7)
    return jnp.stack([top.astype(jnp.bfloat16), (x - top).astype(jnp.bfloat16)])


def split(x):
    top = x.astype(jnp.bfloat16)
    return top, (x - top.astype(F32)).astype(jnp.bfloat16)


def dot(a, b):
    return jnp.dot(a, b, preferred_element_type=F32)


def left_dot(matrix, x):
    top, low = split(x)
    return dot(matrix[0], top) + dot(matrix[1], top) + dot(matrix[0], low)


def right_dot(x, matrix):
    top, low = split(x)
    return dot(top, matrix[0]) + dot(top, matrix[1]) + dot(low, matrix[0])


def squares(x):
    return jnp.sum((x * x).reshape(-1, 8, x.shape[-1]), axis=0)


def pipeline_kernel(
    counts,
    chunk,
    field,
    matrix_a,
    matrix_b,
    matrix_c,
    first,
    mixed,
    twice,
    planes,
    far_field,
    far_mixed,
    sums,
    line,
    made,
    arrived,
    product,
    form,
    mode_a,
    made_a,
    line_send,
    line_recv,
    line_own,
    credit,
    back_send,
    back_recv,
    back_own,
    plane_send,
    plane_recv,
    plane_own,
    home_send,
    home_recv,
    home_own,
    far_send,
    far_recv,
    mixed_send,
    mixed_recv,
    local,
):
    count_x, count_y, count_z = counts
    me_x, me_y, me_z = (lax.axis_index(a) for a in ("gx", "gy", "gz"))
    depth, rows, width = field.shape
    share = depth // count_y
    chunks = rows // chunk
    wide = 2 * chunk
    steps = chunks // 2

    half = count_z // 2
    hub = half - 1
    in_left = me_z < half
    place = jnp.where(in_left, me_z, count_z - 1 - me_z)
    near_hub = jnp.where(in_left, hub, count_z - 1 - hub)
    far_hub = jnp.where(in_left, count_z - 1 - hub, hub)
    is_hub = place == hub

    def seat(m, near):
        return jnp.where(in_left == near, m, count_z - 1 - m) if near else jnp.where(in_left, count_z - 1 - m, m)

    def lines(c, size):
        return pl.ds(pl.multiple_of(c * size, size), size)

    def peer(me, s, count):
        return lax.rem(me + s, count)

    def remote(src, dst, send, recv, axis, to):
        return pltpu.make_async_remote_copy(
            src_ref=src, dst_ref=dst, send_sem=send, recv_sem=recv, device_id={axis: to}, device_id_type=MESH
        )

    barrier = pltpu.get_barrier_semaphore()
    for axis, me, count in (("gx", me_x, count_x), ("gy", me_y, count_y), ("gz", me_z, count_z)):
        for s in range(1, count):
            pl.semaphore_signal(barrier, inc=1, device_id={axis: peer(me, s, count)}, device_id_type=MESH)
    pl.semaphore_wait(barrier, count_x + count_y + count_z - 3)

    def line_far(c):
        return remote(
            field.at[:, lines(c, chunk), :],
            line.at[c % slots, half + place],
            line_send.at[c % slots, 1],
            line_recv.at[c % slots, half + place],
            "gz",
            far_hub,
        )

    def line_near(c):
        return remote(
            field.at[:, lines(c, chunk), :],
            line.at[c % slots, 1 + place],
            line_send.at[c % slots, 0],
            line_recv.at[c % slots, 1 + place],
            "gz",
            near_hub,
        )

    def line_local(c):
        return pltpu.make_async_copy(
            field.at[:, lines(c, chunk), :], line.at[c % slots, 0], line_own.at[c % slots]
        )

    def line_start(c, first_time):
        if not first_time:
            pl.semaphore_wait(credit.at[1], 1)
            line_far(c - slots).wait_send()
        line_far(c).start()

        @pl.when(is_hub)
        def _():
            line_local(c).start()

        if hub > 0:

            @pl.when(jnp.logical_not(is_hub))
            def _():
                if not first_time:
                    pl.semaphore_wait(credit.at[0], 1)
                    line_near(c - slots).wait_send()
                line_near(c).start()

    def line_finish(c):
        line_far(c).wait_send()
        if hub > 0:

            @pl.when(jnp.logical_not(is_hub))
            def _():
                line_near(c).wait_send()

    def back_copy(c, m, e):
        return remote(
            made.at[c % slots, 2 + 2 * m + e],
            (mixed, twice)[e].at[:, lines(c, chunk), :],
            back_send.at[c % slots, m, e],
            back_recv.at[c % ring, e],
            "gz",
            seat(m, True),
        )

    def back_local(c, e):
        return pltpu.make_async_copy(
            made.at[c % slots, e], (mixed, twice)[e].at[:, lines(c, chunk), :], back_own.at[c % slots, e]
        )

    def back_wait(c, e):
        @pl.when(is_hub)
        def _():
            back_local(c, e).wait()
            for m in range(hub):
                back_copy(c, m, e).wait_send()

        if hub > 0:

            @pl.when(jnp.logical_not(is_hub))
            def _():
                back_copy(c, 0, e).wait_recv()

    def line_product(c):
        slot = c % slots
        line_local(c).wait()
        for q in range(1, count_z):
            remote(
                field.at[:, lines(c, chunk), :],
                line.at[slot, q],
                line_send.at[slot, 1],
                line_recv.at[slot, q],
                "gz",
                far_hub,
            ).wait_recv()
        outs = 2 * half
        flat = line.reshape(slots, count_z, depth * chunk, width)
        flat_made = made.reshape(slots, outs, depth * chunk, width)
        for i in range(0, chunk, 2):
            x = jnp.concatenate(
                [
                    jnp.concatenate(
                        [flat[slot, q, pl.ds(i + e, depth, stride=chunk), :] for q in range(count_z)], axis=0
                    )
                    for e in range(2)
                ],
                axis=1,
            )
            y = left_dot(matrix_c, x)
            for r in range(outs):
                for e in range(2):
                    flat_made[slot, r, pl.ds(i + e, depth, stride=chunk), :] = y[
                        r * depth : (r + 1) * depth, e * width : (e + 1) * width
                    ]
        for e in range(2):
            for m in range(hub):
                back_copy(c, m, e).start()
            back_local(c, e).start()

        @pl.when(c + slots < chunks)
        def _():
            for m in range(hub):
                pl.semaphore_signal(credit.at[0], inc=1, device_id={"gz": seat(m, True)}, device_id_type=MESH)
            for m in range(half):
                pl.semaphore_signal(credit.at[1], inc=1, device_id={"gz": seat(m, False)}, device_id_type=MESH)

    def quarter(q):
        return pl.ds(q * share, share)

    def plane_copy(src, c, tick, s):
        to = peer(me_y, s, count_y)
        return remote(
            src.at[quarter(to), lines(c, wide), :],
            arrived.at[me_y, :, lines(c, wide), :],
            plane_send.at[tick % ring, s],
            plane_recv.at[tick % ring, s],
            "gy",
            to,
        )

    def plane_local(src, c, tick):
        return pltpu.make_async_copy(
            src.at[quarter(me_y), lines(c, wide), :],
            arrived.at[me_y, :, lines(c, wide), :],
            plane_own.at[tick % ring],
        )

    def plane_start(src, c, tick):
        for s in range(1, count_y):
            plane_copy(src, c, tick, s).start()
        plane_local(src, c, tick).start()

    def home_copy(phase, c, tick, s):
        to = peer(me_y, s, count_y)
        return remote(
            product.at[tick % hold, to],
            planes.at[phase, quarter(me_y), lines(c, wide), :],
            home_send.at[tick % ring, s],
            home_recv.at[tick % ring, s],
            "gy",
            to,
        )

    def home_local(phase, c, tick):
        return pltpu.make_async_copy(
            product.at[tick % hold, me_y],
            planes.at[phase, quarter(me_y), lines(c, wide), :],
            home_own.at[tick % ring],
        )

    def plane_product(phase, c, tick):
        plane_local(field, c, tick).wait()
        for s in range(1, count_y):
            plane_copy(field, c, tick, s).wait()
        x = jnp.concatenate(
            [arrived[q, :, lines(c, wide), :].reshape(share * wide, width) for q in range(count_y)], axis=1
        )
        y = right_dot(x, matrix_b)
        for q in range(count_y):
            product[tick % hold, q] = y[:, q * width : (q + 1) * width].reshape(share, wide, width)
        for s in range(1, count_y):
            home_copy(phase, c, tick, s).start()
        home_local(phase, c, tick).start()

    def home_wait(phase, c, tick):
        home_local(phase, c, tick).wait()
        for s in range(1, count_y):
            home_copy(phase, c, tick, s).wait()

    def far_copy(s):
        return remote(
            field, far_field.at[s - 1], far_send.at[s - 1], far_recv.at[s - 1], "gx", peer(me_x, s, count_x)
        )

    def far_mixed_copy(c, s):
        return remote(
            mixed.at[:, lines(c, wide), :],
            far_mixed.at[s - 1, :, lines(c, wide), :],
            mixed_send.at[c, s - 1],
            mixed_recv.at[c, s - 1],
            "gx",
            peer(me_x, s, count_x),
        )

    def mode_one_pair(k):
        pair = pl.ds(2 * k, 2)
        loads = [pltpu.make_async_copy(field.at[pair], mode_a.at[0], local.at[0])]
        for s in range(1, count_x):
            loads.append(pltpu.make_async_copy(far_field.at[s - 1, pair], mode_a.at[s], local.at[s]))
        for load in loads:
            load.start()
        for load in loads:
            load.wait()
        sums[0] += squares(mode_a[0])
        x = jnp.concatenate(
            [jnp.concatenate([mode_a[s, e] for s in range(count_x)], axis=0) for e in range(2)], axis=1
        )
        y = left_dot(matrix_a, x)
        for e in range(2):
            made_a[e] = y[:, e * width : (e + 1) * width]
        store = pltpu.make_async_copy(made_a, first.at[pair], local.at[0])
        store.start()
        store.wait()

    def mix(c):
        here = lines(c, wide)
        refs = (first.at[:, here, :], mixed.at[:, here, :], planes.at[0, :, here, :])
        loads = [pltpu.make_async_copy(ref, form.at[e], local.at[e]) for e, ref in enumerate(refs)]
        for load in loads:
            load.start()
        for load in loads:
            load.wait()

        def body(k, total):
            once = form[1, k]
            value = form[0, k] + form[2, k] + once
            form[0, k] = value
            form[1, k] = value + once
            return total + squares(value)

        sums[1] += lax.fori_loop(0, depth, body, jnp.zeros((8, width), F32))
        stores = [pltpu.make_async_copy(form.at[e], refs[e], local.at[e]) for e in range(2)]
        for store in stores:
            store.start()
        for store in stores:
            store.wait()

    for c in range(slots):
        line_start(c, True)
    for s in range(1, count_x):
        far_copy(s).start()
    sums[...] = jnp.zeros_like(sums)

    pairs = depth // 2
    each = pl.cdiv(pairs, steps)

    def valid(tick):
        return ((tick >= 0) & (tick < steps)) | ((tick >= steps + late) & (tick < chunks + late))

    def phase_of(tick):
        return jnp.where(tick < steps, 0, 1)

    def chunk_of(tick):
        return jnp.where(tick < steps, tick, tick - steps - late)

    def tick_body(t, carry):
        @pl.when((t >= late) & (t < chunks + late))
        def _():
            back_wait(t - late, 0)

        @pl.when((t >= slots) & (t < chunks + slots))
        def _():
            back_wait(t - slots, 1)

        @pl.when((t < chunks) & is_hub)
        def _():
            line_product(t)

        @pl.when(t + slots < chunks)
        def _():
            line_start(t + slots, False)

        @pl.when(t < steps)
        def _():
            plane_start(field, t, t)

        @pl.when((t >= steps + late) & (t < chunks + late))
        def _():
            c = t - steps - late
            mix(c)
            plane_start(mixed, c, t)
            for s in range(1, count_x):
                far_mixed_copy(c, s).start()

        ready = t - 4

        @pl.when(valid(ready))
        def _():
            home_wait(phase_of(ready), chunk_of(ready), ready)

        come = t - 2

        @pl.when(valid(come))
        def _():
            plane_product(phase_of(come), chunk_of(come), come)

        @pl.when(t == 1)
        def _():
            for s in range(1, count_x):
                far_copy(s).wait()

        @pl.when((t >= 1) & (t <= steps))
        def _():
            def one(i, carry):
                k = (t - 1) * each + i

                @pl.when(k < pairs)
                def _():
                    mode_one_pair(k)

                return carry

            lax.fori_loop(0, each, one, 0)

        return carry

    lax.fori_loop(0, chunks + late + 4, tick_body, 0)
    for c in range(chunks - slots, chunks):
        line_finish(c)

    def last(c, carry):
        for s in range(1, count_x):
            far_mixed_copy(c, s).wait()
        return carry

    lax.fori_loop(0, steps, last, 0)


def pipeline(field, matrix_a, matrix_b, matrix_c, counts, chunk):
    count_x, count_y, count_z = counts
    depth, rows, width = field.shape
    share = depth // count_y
    steps = rows // chunk // 2
    wide = 2 * chunk
    half = count_z // 2
    anywhere = pl.BlockSpec(memory_space=pl.ANY)
    vmem = pl.BlockSpec(memory_space=pltpu.VMEM)
    block = jax.ShapeDtypeStruct((depth, rows, width), F32)
    far = jax.ShapeDtypeStruct((count_x - 1, depth, rows, width), F32)
    dma = pltpu.SemaphoreType.DMA
    scratch = [
        pltpu.VMEM((slots, count_z, depth, chunk, width), F32),
        pltpu.VMEM((slots, 2 * half, depth, chunk, width), F32),
        pltpu.VMEM((count_y, share, rows, width), F32),
        pltpu.VMEM((hold, count_y, share, wide, width), F32),
        pltpu.VMEM((3, depth, wide, width), F32),
        pltpu.VMEM((count_x, 2, rows, width), F32),
        pltpu.VMEM((2, rows, width), F32),
        dma((slots, 2)),
        dma((slots, count_z)),
        dma((slots,)),
        pltpu.SemaphoreType.REGULAR((2,)),
        dma((slots, max(half - 1, 1), 2)),
        dma((ring, 2)),
        dma((slots, 2)),
        dma((ring, count_y)),
        dma((ring, count_y)),
        dma((ring,)),
        dma((ring, count_y)),
        dma((ring, count_y)),
        dma((ring,)),
        dma((count_x - 1,)),
        dma((count_x - 1,)),
        dma((steps, count_x - 1)),
        dma((steps, count_x - 1)),
        dma((max(count_x, 3),)),
    ]
    return pl.pallas_call(
        functools.partial(pipeline_kernel, counts, chunk),
        in_specs=[anywhere, vmem, vmem, vmem],
        out_specs=[anywhere] * 6 + [vmem],
        out_shape=[
            block,
            block,
            block,
            jax.ShapeDtypeStruct((2, depth, rows, width), F32),
            far,
            far,
            jax.ShapeDtypeStruct((2, 8, width), F32),
        ],
        scratch_shapes=scratch,
        compiler_params=pltpu.CompilerParams(
            collective_id=0, has_side_effects=True, vmem_limit_bytes=64 * 1024 * 1024 - 65536
        ),
        name="pipeline",
    )(field, matrix_a, matrix_b, matrix_c)


def finish_kernel(parts, step, matrix, *refs):
    blocks = refs[:parts]
    planes, twice, field, first, out = refs[parts:]
    pair, rows, width = out.shape
    x = jnp.concatenate(
        [jnp.concatenate([block[k] for block in blocks], axis=0) for k in range(pair)], axis=1
    )
    y = left_dot(matrix, x)
    one = step[0]
    two = one * one / 2.0
    for k in range(pair):
        second = y[:, k * width : (k + 1) * width] + planes[k] + twice[k]
        out[k] = field[k] - one * first[k] + two * second


def finish(step, matrix, mixed, far_mixed, planes, twice, field, first):
    depth, rows, width = field.shape
    count = far_mixed.shape[0]
    pair = 2
    block = pl.BlockSpec((pair, rows, width), lambda k: (k, 0, 0))

    def of(s):
        return pl.BlockSpec((None, pair, rows, width), lambda k: (s, k, 0, 0))

    return pl.pallas_call(
        functools.partial(finish_kernel, 1 + count),
        grid=(depth // pair,),
        in_specs=[
            pl.BlockSpec(memory_space=pltpu.SMEM),
            pl.BlockSpec(matrix.shape, lambda k: (0, 0, 0)),
            block,
            *[of(s) for s in range(count)],
            of(1),
            block,
            block,
            block,
        ],
        out_specs=block,
        out_shape=jax.ShapeDtypeStruct(field.shape, F32),
        name="finish",
    )(step, matrix, mixed, *[far_mixed] * count, planes, twice, field, first)


def line_matrix(factor, count, depth, me):
    half = count // 2
    hub = half - 1
    squared = jnp.dot(factor, factor, precision=lax.Precision.HIGHEST)

    def block(matrix, i, j):
        return matrix[i * depth : (i + 1) * depth, j * depth : (j + 1) * depth]

    def side(mine, theirs):
        return jnp.block(
            [
                [block(matrix, mine[m], w) for w in [mine[hub]] + mine[:hub] + theirs]
                for m in [hub] + list(range(hub))
                for matrix in (factor, squared)
            ]
        )

    left = list(range(half))
    right = list(range(count - 1, half - 1, -1))
    return jnp.where(me < half, side(left, right), side(right, left))


def on_device(field, factor_a, factor_b, factor_c):
    counts = tuple(lax.axis_size(a) for a in ("gx", "gy", "gz"))
    count_x, count_y, count_z = counts
    me_x, me_z = lax.axis_index("gx"), lax.axis_index("gz")
    depth, rows, width = field.shape

    rows_a = lax.dynamic_slice_in_dim(factor_a, me_x * rows, rows, 0)
    matrix_a = jnp.concatenate(
        [
            lax.dynamic_slice_in_dim(rows_a, lax.rem(me_x + count_x - s, count_x) * rows, rows, 1)
            for s in range(count_x)
        ],
        axis=1,
    )

    matrix_c = line_matrix(factor_c, count_z, depth, me_z)
    matrix_a, matrix_b, matrix_c = halves(matrix_a), halves(factor_b.T), halves(matrix_c)

    chunk = min(16, rows // 2)
    first, mixed, twice, planes, _, far_mixed, sums = pipeline(field, matrix_a, matrix_b, matrix_c, counts, chunk)
    sizes = lax.psum(jnp.sum(sums, axis=(1, 2)), ("gx", "gy", "gz"))
    step = target_ratio * jnp.sqrt(sizes[0] / (sizes[1] + epsilon))
    return finish(step[None], matrix_a, mixed, far_mixed, planes, twice, field, first)


def solution(mesh):
    return jax.shard_map(
        on_device,
        mesh=mesh,
        in_specs=(P("gz", "gx", "gy"), P(), P(), P()),
        out_specs=P("gz", "gx", "gy"),
        check_vma=False,
    )
```

```python
import functools

import jax
import jax.numpy as jnp
from jax import lax
from jax.experimental import pallas as pl
from jax.experimental.pallas import tpu as pltpu
from jax.sharding import PartitionSpec as P

epsilon = 1e-06
target_ratio = 0.5
slots = 4
ring = 8
hold = 3
late = 1
F32 = jnp.float32
MESH = pl.DeviceIdType.MESH


def halves(x):
    top = lax.reduce_precision(x, 8, 7)
    return jnp.stack([top.astype(jnp.bfloat16), (x - top).astype(jnp.bfloat16)])


def split(x):
    top = x.astype(jnp.bfloat16)
    return top, (x - top.astype(F32)).astype(jnp.bfloat16)


def dot(a, b):
    return jnp.dot(a, b, preferred_element_type=F32)


def left_dot(matrix, x):
    top, low = split(x)
    return dot(matrix[0], top) + dot(matrix[1], top) + dot(matrix[0], low)


def right_dot(x, matrix):
    top, low = split(x)
    return dot(top, matrix[0]) + dot(top, matrix[1]) + dot(low, matrix[0])


def squares(x):
    return jnp.sum((x * x).reshape(-1, 8, x.shape[-1]), axis=0)


def pipeline_kernel(
    counts,
    chunk,
    field,
    matrix_a,
    matrix_b,
    matrix_c,
    first,
    mixed,
    twice,
    planes,
    far_field,
    far_mixed,
    sums,
    line,
    made,
    arrived,
    product,
    form,
    mode_a,
    made_a,
    line_send,
    line_recv,
    line_own,
    credit,
    back_send,
    back_recv,
    back_own,
    plane_send,
    plane_recv,
    plane_own,
    home_send,
    home_recv,
    home_own,
    far_send,
    far_recv,
    mixed_send,
    mixed_recv,
    local,
    gathered,
    sums_send,
    sums_recv,
):
    count_x, count_y, count_z = counts
    me_x, me_y, me_z = (lax.axis_index(a) for a in ("gx", "gy", "gz"))
    depth, rows, width = field.shape
    share = depth // count_y
    chunks = rows // chunk
    wide = 2 * chunk
    steps = chunks // 2

    half = count_z // 2
    hub = half - 1
    in_left = me_z < half
    place = jnp.where(in_left, me_z, count_z - 1 - me_z)
    near_hub = jnp.where(in_left, hub, count_z - 1 - hub)
    far_hub = jnp.where(in_left, count_z - 1 - hub, hub)
    is_hub = place == hub

    def seat(m, near):
        return jnp.where(in_left == near, m, count_z - 1 - m) if near else jnp.where(in_left, count_z - 1 - m, m)

    def lines(c, size):
        return pl.ds(pl.multiple_of(c * size, size), size)

    def peer(me, s, count):
        return lax.rem(me + s, count)

    def remote(src, dst, send, recv, axis, to):
        return pltpu.make_async_remote_copy(
            src_ref=src, dst_ref=dst, send_sem=send, recv_sem=recv, device_id={axis: to}, device_id_type=MESH
        )

    barrier = pltpu.get_barrier_semaphore()
    for axis, me, count in (("gx", me_x, count_x), ("gy", me_y, count_y), ("gz", me_z, count_z)):
        for s in range(1, count):
            pl.semaphore_signal(barrier, inc=1, device_id={axis: peer(me, s, count)}, device_id_type=MESH)
    pl.semaphore_wait(barrier, count_x + count_y + count_z - 3)

    def line_far(c):
        return remote(
            field.at[:, lines(c, chunk), :],
            line.at[c % slots, half + place],
            line_send.at[c % slots, 1],
            line_recv.at[c % slots, half + place],
            "gz",
            far_hub,
        )

    def line_near(c):
        return remote(
            field.at[:, lines(c, chunk), :],
            line.at[c % slots, 1 + place],
            line_send.at[c % slots, 0],
            line_recv.at[c % slots, 1 + place],
            "gz",
            near_hub,
        )

    def line_local(c):
        return pltpu.make_async_copy(
            field.at[:, lines(c, chunk), :], line.at[c % slots, 0], line_own.at[c % slots]
        )

    def line_start(c, first_time):
        if not first_time:
            pl.semaphore_wait(credit.at[1], 1)
            line_far(c - slots).wait_send()
        line_far(c).start()

        @pl.when(is_hub)
        def _():
            line_local(c).start()

        if hub > 0:

            @pl.when(jnp.logical_not(is_hub))
            def _():
                if not first_time:
                    pl.semaphore_wait(credit.at[0], 1)
                    line_near(c - slots).wait_send()
                line_near(c).start()

    def line_finish(c):
        line_far(c).wait_send()
        if hub > 0:

            @pl.when(jnp.logical_not(is_hub))
            def _():
                line_near(c).wait_send()

    def back_copy(c, m, e):
        return remote(
            made.at[c % slots, 2 + 2 * m + e],
            (mixed, twice)[e].at[:, lines(c, chunk), :],
            back_send.at[c % slots, m, e],
            back_recv.at[c % ring, e],
            "gz",
            seat(m, True),
        )

    def back_local(c, e):
        return pltpu.make_async_copy(
            made.at[c % slots, e], (mixed, twice)[e].at[:, lines(c, chunk), :], back_own.at[c % slots, e]
        )

    def back_wait(c, e):
        @pl.when(is_hub)
        def _():
            back_local(c, e).wait()
            for m in range(hub):
                back_copy(c, m, e).wait_send()

        if hub > 0:

            @pl.when(jnp.logical_not(is_hub))
            def _():
                back_copy(c, 0, e).wait_recv()

    def line_product(c):
        slot = c % slots
        line_local(c).wait()
        for q in range(1, count_z):
            remote(
                field.at[:, lines(c, chunk), :],
                line.at[slot, q],
                line_send.at[slot, 1],
                line_recv.at[slot, q],
                "gz",
                far_hub,
            ).wait_recv()
        outs = 2 * half
        flat = line.reshape(slots, count_z, depth * chunk, width)
        flat_made = made.reshape(slots, outs, depth * chunk, width)
        for i in range(0, chunk, 2):
            x = jnp.concatenate(
                [
                    jnp.concatenate(
                        [flat[slot, q, pl.ds(i + e, depth, stride=chunk), :] for q in range(count_z)], axis=0
                    )
                    for e in range(2)
                ],
                axis=1,
            )
            y = left_dot(matrix_c, x)
            for r in range(outs):
                for e in range(2):
                    flat_made[slot, r, pl.ds(i + e, depth, stride=chunk), :] = y[
                        r * depth : (r + 1) * depth, e * width : (e + 1) * width
                    ]
        for e in range(2):
            for m in range(hub):
                back_copy(c, m, e).start()
            back_local(c, e).start()

        @pl.when(c + slots < chunks)
        def _():
            for m in range(hub):
                pl.semaphore_signal(credit.at[0], inc=1, device_id={"gz": seat(m, True)}, device_id_type=MESH)
            for m in range(half):
                pl.semaphore_signal(credit.at[1], inc=1, device_id={"gz": seat(m, False)}, device_id_type=MESH)

    def quarter(q):
        return pl.ds(q * share, share)

    def plane_copy(src, c, tick, s):
        to = peer(me_y, s, count_y)
        return remote(
            src.at[quarter(to), lines(c, wide), :],
            arrived.at[me_y, :, lines(c, wide), :],
            plane_send.at[tick % ring, s],
            plane_recv.at[tick % ring, s],
            "gy",
            to,
        )

    def plane_local(src, c, tick):
        return pltpu.make_async_copy(
            src.at[quarter(me_y), lines(c, wide), :],
            arrived.at[me_y, :, lines(c, wide), :],
            plane_own.at[tick % ring],
        )

    def plane_start(src, c, tick):
        for s in range(1, count_y):
            plane_copy(src, c, tick, s).start()
        plane_local(src, c, tick).start()

    def home_copy(phase, c, tick, s):
        to = peer(me_y, s, count_y)
        return remote(
            product.at[tick % hold, to],
            planes.at[phase, quarter(me_y), lines(c, wide), :],
            home_send.at[tick % ring, s],
            home_recv.at[tick % ring, s],
            "gy",
            to,
        )

    def home_local(phase, c, tick):
        return pltpu.make_async_copy(
            product.at[tick % hold, me_y],
            planes.at[phase, quarter(me_y), lines(c, wide), :],
            home_own.at[tick % ring],
        )

    def plane_product(phase, c, tick):
        plane_local(field, c, tick).wait()
        for s in range(1, count_y):
            plane_copy(field, c, tick, s).wait()
        x = jnp.concatenate(
            [arrived[q, :, lines(c, wide), :].reshape(share * wide, width) for q in range(count_y)], axis=1
        )
        y = right_dot(x, matrix_b)
        for q in range(count_y):
            product[tick % hold, q] = y[:, q * width : (q + 1) * width].reshape(share, wide, width)
        for s in range(1, count_y):
            home_copy(phase, c, tick, s).start()
        home_local(phase, c, tick).start()

    def home_wait(phase, c, tick):
        home_local(phase, c, tick).wait()
        for s in range(1, count_y):
            home_copy(phase, c, tick, s).wait()

    def far_copy(s):
        return remote(
            field, far_field.at[s - 1], far_send.at[s - 1], far_recv.at[s - 1], "gx", peer(me_x, s, count_x)
        )

    def far_mixed_copy(c, s):
        return remote(
            mixed.at[:, lines(c, wide), :],
            far_mixed.at[s - 1, :, lines(c, wide), :],
            mixed_send.at[c, s - 1],
            mixed_recv.at[c, s - 1],
            "gx",
            peer(me_x, s, count_x),
        )

    def mode_one_pair(k):
        pair = pl.ds(2 * k, 2)
        loads = [pltpu.make_async_copy(field.at[pair], mode_a.at[0], local.at[0])]
        for s in range(1, count_x):
            loads.append(pltpu.make_async_copy(far_field.at[s - 1, pair], mode_a.at[s], local.at[s]))
        for load in loads:
            load.start()
        for load in loads:
            load.wait()
        sums[0] += squares(mode_a[0])
        x = jnp.concatenate(
            [jnp.concatenate([mode_a[s, e] for s in range(count_x)], axis=0) for e in range(2)], axis=1
        )
        y = left_dot(matrix_a, x)
        for e in range(2):
            made_a[e] = y[:, e * width : (e + 1) * width]
        store = pltpu.make_async_copy(made_a, first.at[pair], local.at[0])
        store.start()
        store.wait()

    def mix(c):
        here = lines(c, wide)
        refs = (first.at[:, here, :], mixed.at[:, here, :], planes.at[0, :, here, :])
        loads = [pltpu.make_async_copy(ref, form.at[e], local.at[e]) for e, ref in enumerate(refs)]
        for load in loads:
            load.start()
        for load in loads:
            load.wait()

        def body(k, total):
            once = form[1, k]
            value = form[0, k] + form[2, k] + once
            form[0, k] = value
            form[1, k] = value + once
            return total + squares(value)

        sums[1] += lax.fori_loop(0, depth, body, jnp.zeros((8, width), F32))
        stores = [pltpu.make_async_copy(form.at[e], refs[e], local.at[e]) for e in range(2)]
        for store in stores:
            store.start()
        for store in stores:
            store.wait()

    for c in range(slots):
        line_start(c, True)
    for s in range(1, count_x):
        far_copy(s).start()
    sums[...] = jnp.zeros_like(sums)

    pairs = depth // 2
    each = pl.cdiv(pairs, steps - 1)

    def valid(tick):
        return ((tick >= 0) & (tick < chunks - 1)) | (tick == chunks - 1 + late)

    def phase_of(tick):
        return jnp.where(tick < steps, 0, 1)

    def chunk_of(tick):
        return jnp.where(tick < steps, tick, jnp.minimum(tick - steps, steps - 1))

    axes = (("gx", me_x, count_x), ("gy", me_y, count_y), ("gz", me_z, count_z))

    def sums_copy(a, s):
        axis, me, count = axes[a]
        return remote(
            sums, gathered.at[a, me], sums_send.at[a, s], sums_recv.at[a, s], axis, peer(me, s, count)
        )

    def sums_start(a):
        for s in range(1, axes[a][2]):
            sums_copy(a, s).start()

    def sums_finish(a):
        axis, me, count = axes[a]
        for s in range(1, count):
            sums_copy(a, s).wait()
        gathered[a, me] = sums[...]
        total = gathered[a, 0]
        for q in range(1, count):
            total = total + gathered[a, q]
        sums[...] = total

    def tick_body(t, carry):
        for a in range(3):

            @pl.when(t == chunks + late + a)
            def _():
                sums_finish(a)

        @pl.when((t >= late) & (t < chunks + late))
        def _():
            back_wait(t - late, 0)

        @pl.when((t >= slots) & (t < chunks + slots))
        def _():
            back_wait(t - slots, 1)

        @pl.when((t < chunks) & is_hub)
        def _():
            line_product(t)

        @pl.when(t + slots < chunks)
        def _():
            line_start(t + slots, False)

        @pl.when(t < steps)
        def _():
            plane_start(field, t, t)

        ready = t - 4

        @pl.when(valid(ready))
        def _():
            home_wait(phase_of(ready), chunk_of(ready), ready)

        @pl.when((t >= steps) & valid(t))
        def _():
            c = chunk_of(t)
            mix(c)
            plane_start(mixed, c, t)
            for s in range(1, count_x):
                far_mixed_copy(c, s).start()

        come = t - 2

        @pl.when(valid(come))
        def _():
            plane_product(phase_of(come), chunk_of(come), come)

        @pl.when(t == 1)
        def _():
            for s in range(1, count_x):
                far_copy(s).wait()

        @pl.when((t >= 1) & (t < steps))
        def _():
            def one(i, carry):
                k = (t - 1) * each + i

                @pl.when(k < pairs)
                def _():
                    mode_one_pair(k)

                return carry

            lax.fori_loop(0, each, one, 0)

        for a in range(3):

            @pl.when(t == chunks - 1 + late + a)
            def _():
                sums_start(a)

        return carry

    lax.fori_loop(0, chunks + late + 4, tick_body, 0)
    for c in range(chunks - slots, chunks):
        line_finish(c)

    def last(c, carry):
        for s in range(1, count_x):
            far_mixed_copy(c, s).wait()
        return carry

    lax.fori_loop(0, steps, last, 0)


def pipeline(field, matrix_a, matrix_b, matrix_c, counts, chunk):
    count_x, count_y, count_z = counts
    depth, rows, width = field.shape
    share = depth // count_y
    steps = rows // chunk // 2
    wide = 2 * chunk
    half = count_z // 2
    anywhere = pl.BlockSpec(memory_space=pl.ANY)
    vmem = pl.BlockSpec(memory_space=pltpu.VMEM)
    block = jax.ShapeDtypeStruct((depth, rows, width), F32)
    far = jax.ShapeDtypeStruct((count_x - 1, depth, rows, width), F32)
    dma = pltpu.SemaphoreType.DMA
    scratch = [
        pltpu.VMEM((slots, count_z, depth, chunk, width), F32),
        pltpu.VMEM((slots, 2 * half, depth, chunk, width), F32),
        pltpu.VMEM((count_y, share, rows, width), F32),
        pltpu.VMEM((hold, count_y, share, wide, width), F32),
        pltpu.VMEM((3, depth, wide, width), F32),
        pltpu.VMEM((count_x, 2, rows, width), F32),
        pltpu.VMEM((2, rows, width), F32),
        dma((slots, 2)),
        dma((slots, count_z)),
        dma((slots,)),
        pltpu.SemaphoreType.REGULAR((2,)),
        dma((slots, max(half - 1, 1), 2)),
        dma((ring, 2)),
        dma((slots, 2)),
        dma((ring, count_y)),
        dma((ring, count_y)),
        dma((ring,)),
        dma((ring, count_y)),
        dma((ring, count_y)),
        dma((ring,)),
        dma((count_x - 1,)),
        dma((count_x - 1,)),
        dma((steps, count_x - 1)),
        dma((steps, count_x - 1)),
        dma((max(count_x, 3),)),
        pltpu.VMEM((3, max(counts), 2, 8, width), F32),
        dma((3, max(counts))),
        dma((3, max(counts))),
    ]
    return pl.pallas_call(
        functools.partial(pipeline_kernel, counts, chunk),
        in_specs=[anywhere, vmem, vmem, vmem],
        out_specs=[anywhere] * 6 + [vmem],
        out_shape=[
            block,
            block,
            block,
            jax.ShapeDtypeStruct((2, depth, rows, width), F32),
            far,
            far,
            jax.ShapeDtypeStruct((2, 8, width), F32),
        ],
        scratch_shapes=scratch,
        compiler_params=pltpu.CompilerParams(
            collective_id=0, has_side_effects=True, vmem_limit_bytes=64 * 1024 * 1024 - 65536
        ),
        name="pipeline",
    )(field, matrix_a, matrix_b, matrix_c)


def finish_kernel(parts, step, matrix, *refs):
    blocks = refs[:parts]
    planes, twice, field, first, out = refs[parts:]
    pair, rows, width = out.shape
    x = jnp.concatenate(
        [jnp.concatenate([block[k] for block in blocks], axis=0) for k in range(pair)], axis=1
    )
    y = left_dot(matrix, x)
    one = step[0]
    two = one * one / 2.0
    for k in range(pair):
        second = y[:, k * width : (k + 1) * width] + planes[k] + twice[k]
        out[k] = field[k] - one * first[k] + two * second


def finish(step, matrix, mixed, far_mixed, planes, twice, field, first):
    depth, rows, width = field.shape
    count = far_mixed.shape[0]
    pair = 2
    block = pl.BlockSpec((pair, rows, width), lambda k: (k, 0, 0))

    def of(s):
        return pl.BlockSpec((None, pair, rows, width), lambda k: (s, k, 0, 0))

    return pl.pallas_call(
        functools.partial(finish_kernel, 1 + count),
        grid=(depth // pair,),
        in_specs=[
            pl.BlockSpec(memory_space=pltpu.SMEM),
            pl.BlockSpec(matrix.shape, lambda k: (0, 0, 0)),
            block,
            *[of(s) for s in range(count)],
            of(1),
            block,
            block,
            block,
        ],
        out_specs=block,
        out_shape=jax.ShapeDtypeStruct(field.shape, F32),
        name="finish",
    )(step, matrix, mixed, *[far_mixed] * count, planes, twice, field, first)


def line_matrix(factor, count, depth, me):
    half = count // 2
    hub = half - 1
    squared = jnp.dot(factor, factor, precision=lax.Precision.HIGHEST)

    def block(matrix, i, j):
        return matrix[i * depth : (i + 1) * depth, j * depth : (j + 1) * depth]

    def side(mine, theirs):
        return jnp.block(
            [
                [block(matrix, mine[m], w) for w in [mine[hub]] + mine[:hub] + theirs]
                for m in [hub] + list(range(hub))
                for matrix in (factor, squared)
            ]
        )

    left = list(range(half))
    right = list(range(count - 1, half - 1, -1))
    return jnp.where(me < half, side(left, right), side(right, left))


def on_device(field, factor_a, factor_b, factor_c):
    counts = tuple(lax.axis_size(a) for a in ("gx", "gy", "gz"))
    count_x, count_y, count_z = counts
    me_x, me_z = lax.axis_index("gx"), lax.axis_index("gz")
    depth, rows, width = field.shape

    rows_a = lax.dynamic_slice_in_dim(factor_a, me_x * rows, rows, 0)
    matrix_a = jnp.concatenate(
        [
            lax.dynamic_slice_in_dim(rows_a, lax.rem(me_x + count_x - s, count_x) * rows, rows, 1)
            for s in range(count_x)
        ],
        axis=1,
    )

    matrix_c = line_matrix(factor_c, count_z, depth, me_z)
    matrix_a, matrix_b, matrix_c = halves(matrix_a), halves(factor_b.T), halves(matrix_c)

    chunk = min(16, rows // 4)
    first, mixed, twice, planes, _, far_mixed, sums = pipeline(field, matrix_a, matrix_b, matrix_c, counts, chunk)
    sizes = jnp.sum(sums, axis=(1, 2))
    step = target_ratio * jnp.sqrt(sizes[0] / (sizes[1] + epsilon))
    return finish(step[None], matrix_a, mixed, far_mixed, planes, twice, field, first)


def solution(mesh):
    return jax.shard_map(
        on_device,
        mesh=mesh,
        in_specs=(P("gz", "gx", "gy"), P(), P(), P()),
        out_specs=P("gz", "gx", "gy"),
        check_vma=False,
    )
```

```python
import functools

import jax
import jax.numpy as jnp
from jax import lax
from jax.experimental import pallas as pl
from jax.experimental.pallas import tpu as pltpu
from jax.sharding import PartitionSpec as P

epsilon = 1e-06
target_ratio = 0.5
slots = 4
ring = 8
hold = 3
late = 1
F32 = jnp.float32
MESH = pl.DeviceIdType.MESH


def halves(x):
    top = lax.reduce_precision(x, 8, 7)
    return jnp.stack([top.astype(jnp.bfloat16), (x - top).astype(jnp.bfloat16)])


def split(x):
    top = x.astype(jnp.bfloat16)
    return top, (x - top.astype(F32)).astype(jnp.bfloat16)


def dot(a, b):
    return jnp.dot(a, b, preferred_element_type=F32)


def left_dot(matrix, x):
    top, low = split(x)
    return dot(matrix[0], top) + dot(matrix[1], top) + dot(matrix[0], low)


def right_dot(x, matrix):
    top, low = split(x)
    return dot(top, matrix[0]) + dot(top, matrix[1]) + dot(low, matrix[0])


def squares(x):
    return jnp.sum((x * x).reshape(-1, 8, x.shape[-1]), axis=0)


def pipeline_kernel(
    counts,
    chunk,
    field,
    matrix_a,
    matrix_b,
    matrix_c,
    first,
    mixed,
    twice,
    planes,
    far_field,
    far_mixed,
    sums,
    line,
    made,
    arrived,
    product,
    form,
    mode_a,
    made_a,
    line_send,
    line_recv,
    line_own,
    credit,
    back_send,
    back_recv,
    back_own,
    plane_send,
    plane_recv,
    plane_own,
    home_send,
    home_recv,
    home_own,
    far_send,
    far_recv,
    mixed_send,
    mixed_recv,
    local,
    gathered,
    sums_send,
    sums_recv,
):
    count_x, count_y, count_z = counts
    me_x, me_y, me_z = (lax.axis_index(a) for a in ("gx", "gy", "gz"))
    depth, rows, width = field.shape
    share = depth // count_y
    chunks = rows // chunk
    wide = 2 * chunk
    steps = chunks // 2

    half = count_z // 2
    hub = half - 1
    in_left = me_z < half
    place = jnp.where(in_left, me_z, count_z - 1 - me_z)
    near_hub = jnp.where(in_left, hub, count_z - 1 - hub)
    far_hub = jnp.where(in_left, count_z - 1 - hub, hub)
    is_hub = place == hub

    def seat(m, near):
        return jnp.where(in_left == near, m, count_z - 1 - m) if near else jnp.where(in_left, count_z - 1 - m, m)

    def lines(c, size):
        return pl.ds(pl.multiple_of(c * size, size), size)

    def peer(me, s, count):
        return lax.rem(me + s, count)

    def remote(src, dst, send, recv, axis, to):
        return pltpu.make_async_remote_copy(
            src_ref=src, dst_ref=dst, send_sem=send, recv_sem=recv, device_id={axis: to}, device_id_type=MESH
        )

    barrier = pltpu.get_barrier_semaphore()
    for axis, me, count in (("gx", me_x, count_x), ("gy", me_y, count_y), ("gz", me_z, count_z)):
        for s in range(1, count):
            pl.semaphore_signal(barrier, inc=1, device_id={axis: peer(me, s, count)}, device_id_type=MESH)
    pl.semaphore_wait(barrier, count_x + count_y + count_z - 3)

    def line_far(c):
        return remote(
            field.at[:, lines(c, chunk), :],
            line.at[c % slots, half + place],
            line_send.at[c % slots, 1],
            line_recv.at[c % slots, half + place],
            "gz",
            far_hub,
        )

    def line_near(c):
        return remote(
            field.at[:, lines(c, chunk), :],
            line.at[c % slots, 1 + place],
            line_send.at[c % slots, 0],
            line_recv.at[c % slots, 1 + place],
            "gz",
            near_hub,
        )

    def line_local(c):
        return pltpu.make_async_copy(
            field.at[:, lines(c, chunk), :], line.at[c % slots, 0], line_own.at[c % slots]
        )

    def line_start(c, first_time):
        if not first_time:
            pl.semaphore_wait(credit.at[1], 1)
            line_far(c - slots).wait_send()
        line_far(c).start()

        @pl.when(is_hub)
        def _():
            line_local(c).start()

        if hub > 0:

            @pl.when(jnp.logical_not(is_hub))
            def _():
                if not first_time:
                    pl.semaphore_wait(credit.at[0], 1)
                    line_near(c - slots).wait_send()
                line_near(c).start()

    def line_finish(c):
        line_far(c).wait_send()
        if hub > 0:

            @pl.when(jnp.logical_not(is_hub))
            def _():
                line_near(c).wait_send()

    def back_copy(c, m, e):
        return remote(
            made.at[c % slots, 2 + 2 * m + e],
            (mixed, twice)[e].at[:, lines(c, chunk), :],
            back_send.at[c % slots, m, e],
            back_recv.at[c % ring, e],
            "gz",
            seat(m, True),
        )

    def back_local(c, e):
        return pltpu.make_async_copy(
            made.at[c % slots, e], (mixed, twice)[e].at[:, lines(c, chunk), :], back_own.at[c % slots, e]
        )

    def back_wait(c, e):
        @pl.when(is_hub)
        def _():
            back_local(c, e).wait()
            for m in range(hub):
                back_copy(c, m, e).wait_send()

        if hub > 0:

            @pl.when(jnp.logical_not(is_hub))
            def _():
                back_copy(c, 0, e).wait_recv()

    def line_product(c):
        slot = c % slots
        line_local(c).wait()
        for q in range(1, count_z):
            remote(
                field.at[:, lines(c, chunk), :],
                line.at[slot, q],
                line_send.at[slot, 1],
                line_recv.at[slot, q],
                "gz",
                far_hub,
            ).wait_recv()
        outs = 2 * half
        flat = line.reshape(slots, count_z, depth * chunk, width)
        flat_made = made.reshape(slots, outs, depth * chunk, width)
        for i in range(0, chunk, 2):
            x = jnp.concatenate(
                [
                    jnp.concatenate(
                        [flat[slot, q, pl.ds(i + e, depth, stride=chunk), :] for q in range(count_z)], axis=0
                    )
                    for e in range(2)
                ],
                axis=1,
            )
            y = left_dot(matrix_c, x)
            for r in range(outs):
                for e in range(2):
                    flat_made[slot, r, pl.ds(i + e, depth, stride=chunk), :] = y[
                        r * depth : (r + 1) * depth, e * width : (e + 1) * width
                    ]
        for e in range(2):
            for m in range(hub):
                back_copy(c, m, e).start()
            back_local(c, e).start()

        @pl.when(c + slots < chunks)
        def _():
            for m in range(hub):
                pl.semaphore_signal(credit.at[0], inc=1, device_id={"gz": seat(m, True)}, device_id_type=MESH)
            for m in range(half):
                pl.semaphore_signal(credit.at[1], inc=1, device_id={"gz": seat(m, False)}, device_id_type=MESH)

    def quarter(q):
        return pl.ds(q * share, share)

    def plane_copy(src, c, tick, s):
        to = peer(me_y, s, count_y)
        return remote(
            src.at[quarter(to), lines(c, wide), :],
            arrived.at[me_y, :, lines(c, wide), :],
            plane_send.at[tick % ring, s],
            plane_recv.at[tick % ring, s],
            "gy",
            to,
        )

    def plane_local(src, c, tick):
        return pltpu.make_async_copy(
            src.at[quarter(me_y), lines(c, wide), :],
            arrived.at[me_y, :, lines(c, wide), :],
            plane_own.at[tick % ring],
        )

    def plane_start(src, c, tick):
        for s in range(1, count_y):
            plane_copy(src, c, tick, s).start()
        plane_local(src, c, tick).start()

    def home_copy(phase, c, tick, s):
        to = peer(me_y, s, count_y)
        return remote(
            product.at[tick % hold, to],
            planes.at[phase, quarter(me_y), lines(c, wide), :],
            home_send.at[tick % ring, s],
            home_recv.at[tick % ring, s],
            "gy",
            to,
        )

    def home_local(phase, c, tick):
        return pltpu.make_async_copy(
            product.at[tick % hold, me_y],
            planes.at[phase, quarter(me_y), lines(c, wide), :],
            home_own.at[tick % ring],
        )

    def plane_product(phase, c, tick):
        plane_local(field, c, tick).wait()
        for s in range(1, count_y):
            plane_copy(field, c, tick, s).wait()
        x = jnp.concatenate(
            [arrived[q, :, lines(c, wide), :].reshape(share * wide, width) for q in range(count_y)], axis=1
        )
        y = right_dot(x, matrix_b)
        for q in range(count_y):
            product[tick % hold, q] = y[:, q * width : (q + 1) * width].reshape(share, wide, width)
        for s in range(1, count_y):
            home_copy(phase, c, tick, s).start()
        home_local(phase, c, tick).start()

    def home_wait(phase, c, tick):
        home_local(phase, c, tick).wait()
        for s in range(1, count_y):
            home_copy(phase, c, tick, s).wait()

    def far_copy(s):
        return remote(
            field, far_field.at[s - 1], far_send.at[s - 1], far_recv.at[s - 1], "gx", peer(me_x, s, count_x)
        )

    def far_mixed_copy(c, s):
        return remote(
            mixed.at[:, lines(c, wide), :],
            far_mixed.at[s - 1, :, lines(c, wide), :],
            mixed_send.at[c, s - 1],
            mixed_recv.at[c, s - 1],
            "gx",
            peer(me_x, s, count_x),
        )

    def mode_one_pair(k):
        pair = pl.ds(2 * k, 2)
        loads = [pltpu.make_async_copy(field.at[pair], mode_a.at[0], local.at[0])]
        for s in range(1, count_x):
            loads.append(pltpu.make_async_copy(far_field.at[s - 1, pair], mode_a.at[s], local.at[s]))
        for load in loads:
            load.start()
        for load in loads:
            load.wait()
        sums[0] += squares(mode_a[0])
        x = jnp.concatenate(
            [jnp.concatenate([mode_a[s, e] for s in range(count_x)], axis=0) for e in range(2)], axis=1
        )
        y = left_dot(matrix_a, x)
        for e in range(2):
            made_a[e] = y[:, e * width : (e + 1) * width]
        store = pltpu.make_async_copy(made_a, first.at[pair], local.at[0])
        store.start()
        store.wait()

    def mix(c):
        here = lines(c, wide)
        refs = (first.at[:, here, :], mixed.at[:, here, :], planes.at[0, :, here, :])
        loads = [pltpu.make_async_copy(ref, form.at[e], local.at[e]) for e, ref in enumerate(refs)]
        for load in loads:
            load.start()
        for load in loads:
            load.wait()

        def body(k, total):
            once = form[1, k]
            value = form[0, k] + form[2, k] + once
            form[0, k] = value
            form[1, k] = value + once
            return total + squares(value)

        sums[1] += lax.fori_loop(0, depth, body, jnp.zeros((8, width), F32))
        stores = [pltpu.make_async_copy(form.at[e], refs[e], local.at[e]) for e in range(2)]
        for store in stores:
            store.start()
        for store in stores:
            store.wait()

    for c in range(slots):
        line_start(c, True)
    for s in range(1, count_x):
        far_copy(s).start()
    sums[...] = jnp.zeros_like(sums)

    pairs = depth // 2
    each = pl.cdiv(pairs, steps - 1)

    def valid(tick):
        return ((tick >= 0) & (tick < chunks - 1)) | (tick == chunks - 1 + late)

    def phase_of(tick):
        return jnp.where(tick < steps, 0, 1)

    def chunk_of(tick):
        return jnp.where(tick < steps, tick, jnp.minimum(tick - steps, steps - 1))

    axes = (("gx", me_x, count_x), ("gy", me_y, count_y), ("gz", me_z, count_z))

    def sums_copy(a, s):
        axis, me, count = axes[a]
        return remote(
            sums, gathered.at[a, me], sums_send.at[a, s], sums_recv.at[a, s], axis, peer(me, s, count)
        )

    def sums_start(a):
        for s in range(1, axes[a][2]):
            sums_copy(a, s).start()

    def sums_finish(a):
        axis, me, count = axes[a]
        for s in range(1, count):
            sums_copy(a, s).wait()
        gathered[a, me] = sums[...]
        total = gathered[a, 0]
        for q in range(1, count):
            total = total + gathered[a, q]
        sums[...] = total

    def tick_body(t, carry):
        @pl.when(t < steps)
        def _():
            plane_start(field, t, t)

        come = t - 2

        @pl.when(valid(come))
        def _():
            plane_product(phase_of(come), chunk_of(come), come)

        for a in range(3):

            @pl.when(t == chunks + late + a)
            def _():
                sums_finish(a)

        @pl.when((t >= late) & (t < chunks + late))
        def _():
            back_wait(t - late, 0)

        @pl.when((t >= slots) & (t < chunks + slots))
        def _():
            back_wait(t - slots, 1)

        @pl.when((t < chunks) & is_hub)
        def _():
            line_product(t)

        @pl.when(t + slots < chunks)
        def _():
            line_start(t + slots, False)

        ready = t - 4

        @pl.when(valid(ready))
        def _():
            home_wait(phase_of(ready), chunk_of(ready), ready)

        @pl.when((t >= steps) & valid(t))
        def _():
            c = chunk_of(t)
            mix(c)
            plane_start(mixed, c, t)
            for s in range(1, count_x):
                far_mixed_copy(c, s).start()

        @pl.when(t == 1)
        def _():
            for s in range(1, count_x):
                far_copy(s).wait()

        @pl.when((t >= 1) & (t < steps))
        def _():
            def one(i, carry):
                k = (t - 1) * each + i

                @pl.when(k < pairs)
                def _():
                    mode_one_pair(k)

                return carry

            lax.fori_loop(0, each, one, 0)

        for a in range(3):

            @pl.when(t == chunks - 1 + late + a)
            def _():
                sums_start(a)

        return carry

    lax.fori_loop(0, chunks + late + 4, tick_body, 0)
    for c in range(chunks - slots, chunks):
        line_finish(c)

    def last(c, carry):
        for s in range(1, count_x):
            far_mixed_copy(c, s).wait()
        return carry

    lax.fori_loop(0, steps, last, 0)


def pipeline(field, matrix_a, matrix_b, matrix_c, counts, chunk):
    count_x, count_y, count_z = counts
    depth, rows, width = field.shape
    share = depth // count_y
    steps = rows // chunk // 2
    wide = 2 * chunk
    half = count_z // 2
    anywhere = pl.BlockSpec(memory_space=pl.ANY)
    vmem = pl.BlockSpec(memory_space=pltpu.VMEM)
    block = jax.ShapeDtypeStruct((depth, rows, width), F32)
    far = jax.ShapeDtypeStruct((count_x - 1, depth, rows, width), F32)
    dma = pltpu.SemaphoreType.DMA
    scratch = [
        pltpu.VMEM((slots, count_z, depth, chunk, width), F32),
        pltpu.VMEM((slots, 2 * half, depth, chunk, width), F32),
        pltpu.VMEM((count_y, share, rows, width), F32),
        pltpu.VMEM((hold, count_y, share, wide, width), F32),
        pltpu.VMEM((3, depth, wide, width), F32),
        pltpu.VMEM((count_x, 2, rows, width), F32),
        pltpu.VMEM((2, rows, width), F32),
        dma((slots, 2)),
        dma((slots, count_z)),
        dma((slots,)),
        pltpu.SemaphoreType.REGULAR((2,)),
        dma((slots, max(half - 1, 1), 2)),
        dma((ring, 2)),
        dma((slots, 2)),
        dma((ring, count_y)),
        dma((ring, count_y)),
        dma((ring,)),
        dma((ring, count_y)),
        dma((ring, count_y)),
        dma((ring,)),
        dma((count_x - 1,)),
        dma((count_x - 1,)),
        dma((steps, count_x - 1)),
        dma((steps, count_x - 1)),
        dma((max(count_x, 3),)),
        pltpu.VMEM((3, max(counts), 2, 8, width), F32),
        dma((3, max(counts))),
        dma((3, max(counts))),
    ]
    return pl.pallas_call(
        functools.partial(pipeline_kernel, counts, chunk),
        in_specs=[anywhere, vmem, vmem, vmem],
        out_specs=[anywhere] * 6 + [vmem],
        out_shape=[
            block,
            block,
            block,
            jax.ShapeDtypeStruct((2, depth, rows, width), F32),
            far,
            far,
            jax.ShapeDtypeStruct((2, 8, width), F32),
        ],
        scratch_shapes=scratch,
        compiler_params=pltpu.CompilerParams(
            collective_id=0, has_side_effects=True, vmem_limit_bytes=64 * 1024 * 1024 - 65536
        ),
        name="pipeline",
    )(field, matrix_a, matrix_b, matrix_c)


def finish_kernel(parts, step, matrix, *refs):
    blocks = refs[:parts]
    planes, twice, field, first, out = refs[parts:]
    pair, rows, width = out.shape
    x = jnp.concatenate(
        [jnp.concatenate([block[k] for block in blocks], axis=0) for k in range(pair)], axis=1
    )
    y = left_dot(matrix, x)
    one = step[0]
    two = one * one / 2.0
    for k in range(pair):
        second = y[:, k * width : (k + 1) * width] + planes[k] + twice[k]
        out[k] = field[k] - one * first[k] + two * second


def finish(step, matrix, mixed, far_mixed, planes, twice, field, first):
    depth, rows, width = field.shape
    count = far_mixed.shape[0]
    pair = 2
    block = pl.BlockSpec((pair, rows, width), lambda k: (k, 0, 0))

    def of(s):
        return pl.BlockSpec((None, pair, rows, width), lambda k: (s, k, 0, 0))

    return pl.pallas_call(
        functools.partial(finish_kernel, 1 + count),
        grid=(depth // pair,),
        in_specs=[
            pl.BlockSpec(memory_space=pltpu.SMEM),
            pl.BlockSpec(matrix.shape, lambda k: (0, 0, 0)),
            block,
            *[of(s) for s in range(count)],
            of(1),
            block,
            block,
            block,
        ],
        out_specs=block,
        out_shape=jax.ShapeDtypeStruct(field.shape, F32),
        name="finish",
    )(step, matrix, mixed, *[far_mixed] * count, planes, twice, field, first)


def line_matrix(factor, count, depth, me):
    half = count // 2
    hub = half - 1
    squared = jnp.dot(factor, factor, precision=lax.Precision.HIGHEST)

    def block(matrix, i, j):
        return matrix[i * depth : (i + 1) * depth, j * depth : (j + 1) * depth]

    def side(mine, theirs):
        return jnp.block(
            [
                [block(matrix, mine[m], w) for w in [mine[hub]] + mine[:hub] + theirs]
                for m in [hub] + list(range(hub))
                for matrix in (factor, squared)
            ]
        )

    left = list(range(half))
    right = list(range(count - 1, half - 1, -1))
    return jnp.where(me < half, side(left, right), side(right, left))


def on_device(field, factor_a, factor_b, factor_c):
    counts = tuple(lax.axis_size(a) for a in ("gx", "gy", "gz"))
    count_x, count_y, count_z = counts
    me_x, me_z = lax.axis_index("gx"), lax.axis_index("gz")
    depth, rows, width = field.shape

    rows_a = lax.dynamic_slice_in_dim(factor_a, me_x * rows, rows, 0)
    matrix_a = jnp.concatenate(
        [
            lax.dynamic_slice_in_dim(rows_a, lax.rem(me_x + count_x - s, count_x) * rows, rows, 1)
            for s in range(count_x)
        ],
        axis=1,
    )

    matrix_c = line_matrix(factor_c, count_z, depth, me_z)
    matrix_a, matrix_b, matrix_c = halves(matrix_a), halves(factor_b.T), halves(matrix_c)

    chunk = min(16, rows // 4)
    first, mixed, twice, planes, _, far_mixed, sums = pipeline(field, matrix_a, matrix_b, matrix_c, counts, chunk)
    sizes = jnp.sum(sums, axis=(1, 2))
    step = target_ratio * jnp.sqrt(sizes[0] / (sizes[1] + epsilon))
    return finish(step[None], matrix_a, mixed, far_mixed, planes, twice, field, first)


def solution(mesh):
    return jax.shard_map(
        on_device,
        mesh=mesh,
        in_specs=(P("gz", "gx", "gy"), P(), P(), P()),
        out_specs=P("gz", "gx", "gy"),
        check_vma=False,
    )
```
